32 devices in a mesh: zero: 8 (over z, x), model: 4 (over y, core).
Axes of the slice: x: 2, y: 2, z: 4, core: 2. Of those that a mesh axis runs over, the one named last changes fastest.
Arguments:
- train_up: bfloat16 [12288, 49152], P('zero', 'model'), may hold values from -0.078125 to 0.078125
- low_up: bfloat16 [12288, 32], P('zero'), may hold values from -0.0546875 to 0.0546875
- high_up: bfloat16 [32, 49152], P(None, 'model'), may hold values from -1 to 1
- norm_train: float32 [12288], P(('zero', 'model')), may hold values from 0.25 to 1.75
- norm_step: float32 [12288], P(('zero', 'model')), may hold values from -0.3 to 0.3
Outputs:
- serving_up: bfloat16 [12288, 49152], P(None, ('model', 'zero'))
- scale_up: float32 [49152], P(('model', 'zero'))
- serve_norm: bfloat16 [12288], replicated
The draws below stay inside these ranges and needn't reach their ends.
All inputs are finite; a program needn't handle non-finite values. Where the reference program divides by a largest or mean magnitude, that divisor is 1e-20 or more.
Results may differ from the reference program's by a relative error of at most 0.001.
Values may be sent and summed in bfloat16 or wider, within the bound.
A program may use at most 192 MiB of HBM per device.

```python
import jax
import jax.numpy as jnp

D_MODEL = 12288
D_INNER = 49152
RANK = 32


def with_spikes(result, own_key, source, target, parts, factor):
    def block_of(dim):
        return (jnp.arange(result.shape[dim]) // (result.shape[dim] // parts)).reshape((-1,) + (1,) * (result.ndim - 1 - dim))

    near = jax.random.permutation(own_key, parts)[block_of(target)]
    far = (block_of(target) + parts // 2) % parts
    return jnp.where((block_of(source) == near) | (block_of(source) == far), factor * result, result)


def steps_of(rng, shape, shards, smallest, high):
    loudness, own = 1.0, jax.random.fold_in(rng, 6)
    for axis_at, parts in shards:
        draws = jnp.exp(jax.random.uniform(jax.random.fold_in(own, axis_at), (parts,), jnp.float32, smallest / len(shards), high / len(shards)))
        loudness = loudness * jnp.repeat(draws, shape[axis_at] // parts).reshape([-1 if axis == axis_at else 1 for axis in range(len(shape))])
    return loudness


def bell_draw(rng, dims, scale, limit, pieces=(), dtype=jnp.bfloat16):
    drawn = scale * jax.random.normal(rng, dims, jnp.float32)
    if pieces:
        drawn = drawn * steps_of(rng, dims, pieces, -0.22, 0.18)
    return jnp.clip(drawn, -limit, limit).astype(dtype)


def gaussian_with(key, shape, spread, reach, cuts, heavy, dtype=jnp.bfloat16):
    array = spread * jax.random.normal(key, shape, jnp.float32)
    if cuts:
        array = array * steps_of(key, shape, cuts, -0.22, 0.18)
    return jnp.clip(with_spikes(array, jax.random.fold_in(key, 3), *heavy), -reach, reach).astype(dtype)


def setup_inputs(seed: int = 0) -> dict:
    splits = jax.random.split(jax.random.key(seed), 6)
    train_up = gaussian_with(splits[0], (D_MODEL, D_INNER), D_MODEL ** -0.5, 0.078125, ((0, 8), (1, 4)), (0, 1, 8, 2.0))
    low_up = bell_draw(splits[1], (D_MODEL, RANK), D_MODEL ** -0.5, 0.0546875, ((0, 8),))
    high_up = bell_draw(splits[2], (RANK, D_INNER), RANK ** -0.5, 1.0, ((1, 4),))
    norm_train = jnp.clip(1.0 + 0.15 * jax.random.normal(splits[3], (D_MODEL,), jnp.float32), 0.25, 1.75)
    norm_step = jnp.clip(jax.random.uniform(splits[4], (D_MODEL,), jnp.float32, -0.3, 0.3) * steps_of(splits[4], (D_MODEL,), ((0, 32),), -0.4, 0.0), -0.3, 0.3)
    return {"train_up": train_up, "low_up": low_up, "high_up": high_up, "norm_train": norm_train, "norm_step": norm_step}


mix_rate = 0.5


def reference(train_up, low_up, high_up, norm_train, norm_step):
    whole_up = train_up.astype(jnp.float32) + mix_rate * jnp.dot(low_up, high_up, preferred_element_type=jnp.float32)
    scale_up = jnp.sum(jnp.abs(whole_up), axis=0) / D_MODEL
    serving_up = (whole_up / scale_up).astype(jnp.bfloat16)
    serve_norm = (norm_train + norm_step).astype(jnp.bfloat16)
    return serving_up, scale_up, serve_norm
```

```python
import functools

import jax
import jax.numpy as jnp
from jax import lax
from jax.experimental import pallas as pl
from jax.experimental.pallas import tpu as pltpu
from jax.sharding import PartitionSpec as P

mix_rate = 0.5
MESH = pl.DeviceIdType.MESH
GRANT = 22 * 2**20


def bit(value, place):
    return lax.rem(lax.div(value, 2**place), 2)


def partner(me, key, n):
    other = 0
    for place in range(n.bit_length() - 1):
        a, b = bit(me, place), bit(key, place)
        other = other + 2**place * (a + b - 2 * a * b)
    return other


def send_order(n):
    far = list(range(n // 2, n))
    near = list(range(n // 2 - 1, 0, -1))
    order = []
    for i in range(len(far)):
        order.append(far[i])
        if i < len(near):
            order.append(near[i])
    return order


def orders(n):
    if n == 8:
        sends = ([6, 7, 4, 5, 2, 3, 1], [1, 2, 3, 4, 5, 6, 7])
        waits = ([6, 7, 2, 3, 1, 4, 5], [1, 4, 5, 2, 3, 6, 7])
        return sends, waits
    order = send_order(n)
    return (order, order), (order, order)


def key_at(order, place, middle):
    ends, mids = order[0][place], order[1][place]
    return ends if ends == mids else ends + middle * (mids - ends)


def exchange(n, m, q, cw, train, low, high, gain, whole, scale, norm, lows, norms, highs, w, sends, recvs, low_s, low_r, norm_s, norm_r, side_s, side_r, mine):
    me = lax.axis_index("zero")
    lane = lax.axis_index("model")
    rows = train.shape[0]
    cols = whole.shape[1]
    pieces = cols // cw
    share = rows // q
    z = lax.div(me, 2)
    middle = lax.rem(lax.div(z, 2) + z, 2)
    send_keys, wait_keys = orders(n)
    peers = [partner(me, key_at(send_keys, p, middle), n) for p in range(n - 1)]
    sources = [partner(me, key_at(wait_keys, p, middle), n) for p in range(n - 1)]
    sides = [lax.rem(lane + k, m) for k in range(1, m)]

    barrier = pltpu.get_barrier_semaphore()
    for peer in peers:
        pl.semaphore_signal(barrier, inc=1, device_id={"zero": peer}, device_id_type=MESH)
    for side in sides:
        pl.semaphore_signal(barrier, inc=1, device_id={"model": side}, device_id_type=MESH)

    own = [
        pltpu.make_async_copy(train.at[:, pl.ds(pl.multiple_of(me * cols, 128), cols)], whole.at[pl.ds(pl.multiple_of(me * rows, 128), rows), :], mine.at[0]),
        pltpu.make_async_copy(high.at[:, pl.ds(pl.multiple_of(me * cols, 128), cols)], highs, mine.at[1]),
    ]
    at = lane if q > 1 else 0
    low_part = low.at[:, pl.ds(pl.multiple_of(at * share, 128), share)]
    keep = [
        pltpu.make_async_copy(low_part, lows.at[at, me], mine.at[2]),
        pltpu.make_async_copy(gain, norms.at[lane, me], mine.at[3]),
    ]
    for copy in keep + own:
        copy.start()
    pl.semaphore_wait(barrier, n + m - 2)

    def low_copy(origin, peer):
        return pltpu.make_async_remote_copy(
            src_ref=low_part, dst_ref=lows.at[at, origin], send_sem=low_s.at[peer], recv_sem=low_r.at[origin], device_id={"zero": peer}, device_id_type=MESH
        )

    def norm_copy(origin, peer):
        return pltpu.make_async_remote_copy(
            src_ref=gain, dst_ref=norms.at[lane, origin], send_sem=norm_s.at[peer], recv_sem=norm_r.at[origin], device_id={"zero": peer}, device_id_type=MESH
        )

    def block_copy(origin, peer, c):
        return pltpu.make_async_remote_copy(
            src_ref=train.at[:, pl.ds(pl.multiple_of(peer * cols + c * cw, 128), cw)],
            dst_ref=whole.at[pl.ds(pl.multiple_of(origin * rows, 128), rows), pl.ds(pl.multiple_of(c * cw, 128), cw)],
            send_sem=sends.at[peer, c],
            recv_sem=recvs.at[origin, c],
            device_id={"zero": peer},
            device_id_type=MESH,
        )

    def side_copies(origin, side):
        pairs = [(norms.at[origin], norms.at[origin])]
        if q > 1:
            pairs.append((lows.at[origin], lows.at[origin]))
        return [
            pltpu.make_async_remote_copy(src_ref=src, dst_ref=dst, send_sem=side_s.at[i, side], recv_sem=side_r.at[i, origin], device_id={"model": side}, device_id_type=MESH)
            for i, (src, dst) in enumerate(pairs)
        ]

    for peer in peers:
        low_copy(me, peer).start()
        norm_copy(me, peer).start()
    for peer in peers:
        for c in range(pieces):
            block_copy(me, peer, c).start()

    for copy in keep + own:
        copy.wait()
    for source in sources:
        low_copy(source, source).wait_recv()
        norm_copy(source, source).wait_recv()
    for side in sides:
        for copy in side_copies(lane, side):
            copy.start()
    highs[...] = (mix_rate * highs[...].astype(jnp.float32)).astype(highs.dtype)
    for side in sides:
        for copy in side_copies(side, side):
            copy.wait_recv()

    for i in range(n):
        for j in range(m):
            norm[i, j] = norms[j, i]

    tall = 128
    per = share // tall
    far = 256 if rows % 256 == 0 else 128

    def piece(c, carry):
        columns = pl.ds(pl.multiple_of(c * cw, 128), cw)
        high_tile = highs[:, columns]

        def block(origin, total):
            def add_up(t, total):
                a = pl.multiple_of(origin * rows + t * tall, tall)
                part = lows[lax.div(t, per), origin, :, pl.ds(pl.multiple_of(lax.rem(t, per) * tall, tall), tall)]
                extra = lax.dot_general(part, high_tile, (((0,), (0,)), ((), ())), preferred_element_type=jnp.float32)
                new = whole[pl.ds(a, tall), columns].astype(jnp.float32) + extra
                w[pl.ds(a, tall), :] = new
                return total + jnp.sum(jnp.abs(new).reshape(tall // 8, 8, cw), axis=0)

            return lax.fori_loop(0, rows // tall, add_up, total, unroll=3)

        total = block(me, jnp.zeros((8, cw), jnp.float32))
        for source in sources:
            block_copy(source, source, c).wait_recv()
            total = block(source, total)
        mean = jnp.sum(total, axis=0, keepdims=True) / (n * rows)
        scale[:, columns] = mean
        inverse = 1.0 / mean

        def divide(t, carry):
            a = pl.multiple_of(t * far, far)
            whole[pl.ds(a, far), columns] = (w[pl.ds(a, far), :] * inverse).astype(whole.dtype)
            return carry

        lax.fori_loop(0, n * rows // far, divide, 0, unroll=2)
        return carry

    lax.fori_loop(0, pieces, piece, 0)

    for peer in peers:
        low_copy(me, peer).wait_send()
        norm_copy(me, peer).wait_send()
        for c in range(pieces):
            block_copy(me, peer, c).wait_send()
    for side in sides:
        for copy in side_copies(lane, side):
            copy.wait_send()


def gather_and_serve(n, m, train, low, high, gain):
    rows, width = train.shape
    cols = width // n
    rank = low.shape[0]
    piece = gain.shape[1]
    q = m if rows % (128 * m) == 0 else 1
    cw = 256 if cols % 256 == 0 else 128
    pieces = cols // cw
    dma = pltpu.SemaphoreType.DMA
    return pl.pallas_call(
        functools.partial(exchange, n, m, q, cw),
        out_shape=(
            pltpu.VMEM((n * rows, cols), train.dtype),
            pltpu.VMEM((1, cols), jnp.float32),
            pltpu.VMEM((n, m, 1, piece), jnp.float32),
        ),
        in_specs=[pl.BlockSpec(memory_space=pl.ANY)] * 4,
        out_specs=[pl.BlockSpec(memory_space=pltpu.VMEM)] * 3,
        scratch_shapes=[
            pltpu.VMEM((q, n, rank, rows // q), low.dtype),
            pltpu.VMEM((m, n, 1, piece), jnp.float32),
            pltpu.VMEM((rank, cols), high.dtype),
            pltpu.VMEM((n * rows, cw), jnp.float32),
            dma((n, pieces)),
            dma((n, pieces)),
            dma((n,)),
            dma((n,)),
            dma((n,)),
            dma((n,)),
            dma((2, m)),
            dma((2, m)),
            dma((4,)),
        ],
        compiler_params=pltpu.CompilerParams(collective_id=0, has_side_effects=True, vmem_limit_bytes=GRANT),
        name="exchange",
    )(train, low, high, gain)


def put_out(parts, whole, serving, sems):
    tall = whole.shape[0] // parts
    copies = [pltpu.make_async_copy(whole.at[pl.ds(i * tall, tall), :], serving.at[pl.ds(i * tall, tall), :], sems.at[i]) for i in range(parts)]
    for copy in copies:
        copy.start()
    for copy in copies:
        copy.wait()


def store(whole):
    parts = 12
    return pl.pallas_call(
        functools.partial(put_out, parts),
        out_shape=jax.ShapeDtypeStruct(whole.shape, whole.dtype),
        in_specs=[pl.BlockSpec(memory_space=pl.ANY)],
        out_specs=pl.BlockSpec(memory_space=pl.ANY),
        scratch_shapes=[pltpu.SemaphoreType.DMA((parts,))],
        compiler_params=pltpu.CompilerParams(vmem_limit_bytes=GRANT),
        name="store",
    )(pltpu.with_memory_space_constraint(whole, pltpu.VMEM))


def local(n, m, train_up, low_up, high_up, norm_train, norm_step):
    gain = (norm_train + norm_step).reshape(1, -1)
    whole, scale, norm = gather_and_serve(n, m, train_up, low_up.T, high_up, gain)
    return (store(whole), scale.reshape(-1), norm.reshape(-1).astype(jnp.bfloat16))


def solution(mesh):
    in_specs = (
        P("zero", "model"),
        P("zero", None),
        P(None, "model"),
        P(("zero", "model")),
        P(("zero", "model")),
    )
    out_specs = (P(None, ("model", "zero")), P(("model", "zero")), P())
    body = functools.partial(local, mesh.shape["zero"], mesh.shape["model"])
    return jax.shard_map(body, mesh=mesh, in_specs=in_specs, out_specs=out_specs, check_vma=False)
```

```python
import functools

import jax
import jax.numpy as jnp
from jax import lax
from jax.experimental import pallas as pl
from jax.experimental.pallas import tpu as pltpu
from jax.sharding import PartitionSpec as P

mix_rate = 0.5
MESH = pl.DeviceIdType.MESH
GRANT = 16 * 2**20
HELD = (6, 7)
CROSS = (2, 3, 4, 5)
LEAD = 3


def bit(value, place):
    return lax.rem(lax.div(value, 2**place), 2)


def partner(me, key, n):
    other = 0
    for place in range(n.bit_length() - 1):
        a, b = bit(me, place), bit(key, place)
        other = other + 2**place * (a + b - 2 * a * b)
    return other


def send_order(n):
    far = list(range(n // 2, n))
    near = list(range(n // 2 - 1, 0, -1))
    order = []
    for i in range(len(far)):
        order.append(far[i])
        if i < len(near):
            order.append(near[i])
    return order


def orders(n):
    if n == 8:
        sends = ([6, 7, 4, 5, 2, 3, 1], [1, 2, 3, 4, 5, 6, 7])
        waits = ([6, 7, 2, 3, 1, 4, 5], [1, 4, 5, 2, 3, 6, 7])
        return sends, waits
    order = send_order(n)
    return (order, order), (order, order)


def key_at(order, place, middle):
    ends, mids = order[0][place], order[1][place]
    return ends if ends == mids else ends + middle * (mids - ends)


def is_held(n, order, place):
    return n == 8 and order[0][place] in HELD


def exchange(n, m, q, cw, train, low, high, gain, whole, scale, norm, total_out, w_out, lows, norms, highs, w, sends, recvs, low_s, low_r, norm_s, norm_r, side_s, side_r, mine, go):
    me = lax.axis_index("zero")
    lane = lax.axis_index("model")
    rows = train.shape[0]
    cols = whole.shape[1]
    pieces = cols // cw
    share = rows // q
    z = lax.div(me, 2)
    middle = lax.rem(lax.div(z, 2) + z, 2)
    send_keys, wait_keys = orders(n)
    peers = [partner(me, key_at(send_keys, p, middle), n) for p in range(n - 1)]
    sources = [partner(me, key_at(wait_keys, p, middle), n) for p in range(n - 1)]
    sides = [lax.rem(lane + k, m) for k in range(1, m)]

    barrier = pltpu.get_barrier_semaphore()
    for peer in peers:
        pl.semaphore_signal(barrier, inc=1, device_id={"zero": peer}, device_id_type=MESH)
    for side in sides:
        pl.semaphore_signal(barrier, inc=1, device_id={"model": side}, device_id_type=MESH)

    own = [
        pltpu.make_async_copy(train.at[:, pl.ds(pl.multiple_of(me * cols, 128), cols)], whole.at[pl.ds(pl.multiple_of(me * rows, 128), rows), :], mine.at[0]),
        pltpu.make_async_copy(high.at[:, pl.ds(pl.multiple_of(me * cols, 128), cols)], highs, mine.at[1]),
    ]
    at = lane if q > 1 else 0
    low_part = low.at[:, pl.ds(pl.multiple_of(at * share, 128), share)]
    keep = [
        pltpu.make_async_copy(low_part, lows.at[at, me], mine.at[2]),
        pltpu.make_async_copy(gain, norms.at[lane, me], mine.at[3]),
    ]
    for copy in keep + own:
        copy.start()
    pl.semaphore_wait(barrier, n + m - 2)

    def spread(i, origin, peer, fresh):
        refs = ((low_part, lows.at[at, origin], low_s, low_r), (gain, norms.at[lane, origin], norm_s, norm_r))
        return [
            pltpu.make_async_remote_copy(
                src_ref=src if fresh else dst, dst_ref=dst, send_sem=sent.at[i], recv_sem=came.at[origin], device_id={"zero": peer}, device_id_type=MESH
            )
            for src, dst, sent, came in refs
        ]

    def block_copy(origin, peer, c):
        return pltpu.make_async_remote_copy(
            src_ref=train.at[:, pl.ds(pl.multiple_of(peer * cols + c * cw, 128), cw)],
            dst_ref=whole.at[pl.ds(pl.multiple_of(origin * rows, 128), rows), pl.ds(pl.multiple_of(c * cw, 128), cw)],
            send_sem=sends.at[peer, c],
            recv_sem=recvs.at[origin, c],
            device_id={"zero": peer},
            device_id_type=MESH,
        )

    def side_copies(origin, side):
        pairs = [(norms.at[origin], norms.at[origin])]
        if q > 1:
            pairs.append((lows.at[origin], lows.at[origin]))
        return [
            pltpu.make_async_remote_copy(src_ref=src, dst_ref=dst, send_sem=side_s.at[i, side], recv_sem=side_r.at[i, origin], device_id={"model": side}, device_id_type=MESH)
            for i, (src, dst) in enumerate(pairs)
        ]

    spreads = spread(0, me, partner(me, n // 2, n), True)
    for copy in spreads:
        copy.start()
    last = pieces - 1
    for p, peer in enumerate(peers):
        for c in range(pieces):
            if c == last and is_held(n, send_keys, p):

                @pl.when(middle == 1)
                def _():
                    block_copy(me, peer, c).start()

            else:
                block_copy(me, peer, c).start()

    for copy in keep + own:
        copy.wait()
    held = [me]
    key = n // 2
    while key:
        peer = partner(me, key, n)
        if key < n // 2:
            for origin in held:
                copies = spread(len(spreads) // 2, origin, peer, False)
                for copy in copies:
                    copy.start()
                spreads += copies
        arrived = [partner(origin, key, n) for origin in held]
        for origin in arrived:
            for copy in spread(0, origin, peer, False):
                copy.wait_recv()
        held += arrived
        key //= 2
    for side in sides:
        for copy in side_copies(lane, side):
            copy.start()
    highs[...] = (mix_rate * highs[...].astype(jnp.float32)).astype(highs.dtype)
    for side in sides:
        for copy in side_copies(side, side):
            copy.wait_recv()

    for i in range(n):
        for j in range(m):
            norm[i, j] = norms[j, i]

    tall = 128
    per = share // tall
    far = 256 if rows % 256 == 0 else 128

    def merge(origin, columns, total, landed=True):
        high_tile = highs[:, columns]

        def add_up(t, total):
            a = pl.multiple_of(origin * rows + t * tall, tall)
            part = lows[lax.div(t, per), origin, :, pl.ds(pl.multiple_of(lax.rem(t, per) * tall, tall), tall)]
            new = lax.dot_general(part, high_tile, (((0,), (0,)), ((), ())), preferred_element_type=jnp.float32)
            if landed:
                new = whole[pl.ds(a, tall), columns].astype(jnp.float32) + new
            w[pl.ds(a, tall), :] = new
            return total + jnp.sum(jnp.abs(new).reshape(tall // 8, 8, cw), axis=0) if landed else total

        return lax.fori_loop(0, rows // tall, add_up, total, unroll=3)

    def finish_columns(columns, total):
        mean = jnp.sum(total, axis=0, keepdims=True) / (n * rows)
        scale[:, columns] = mean
        inverse = 1.0 / mean

        def divide(t, carry):
            a = pl.multiple_of(t * far, far)
            whole[pl.ds(a, far), columns] = (w[pl.ds(a, far), :] * inverse).astype(whole.dtype)
            return carry

        lax.fori_loop(0, n * rows // far, divide, 0, unroll=2)

    def piece(c, carry):
        columns = pl.ds(pl.multiple_of(c * cw, 128), cw)
        total = merge(me, columns, jnp.zeros((8, cw), jnp.float32))
        for source in sources:
            block_copy(source, source, c).wait_recv()
            total = merge(source, columns, total)
        if n == 8:

            @pl.when(jnp.logical_and(middle == 1, c == pieces - LEAD))
            def _():
                for key in CROSS:
                    pl.semaphore_signal(go, inc=1, device_id={"zero": partner(me, key, n)}, device_id_type=MESH)

        finish_columns(columns, total)
        return carry

    if n != 8:
        lax.fori_loop(0, pieces, piece, 0)
        total_out[...] = jnp.zeros_like(total_out)
    else:
        lax.fori_loop(0, last, piece, 0)
        columns = pl.ds(last * cw, cw)
        total = merge(me, columns, jnp.zeros((8, cw), jnp.float32))
        held = [source for p, source in enumerate(sources) if is_held(n, wait_keys, p)]
        for p, source in enumerate(sources):
            if not is_held(n, wait_keys, p):
                block_copy(source, source, last).wait_recv()
                total = merge(source, columns, total)
        total_out[...] = total

        @pl.when(middle == 1)
        def _():
            total = total_out[...]
            for source in held:
                block_copy(source, source, last).wait_recv()
                total = merge(source, columns, total)
            finish_columns(columns, total)

        @pl.when(middle == 0)
        def _():
            for source in held:
                merge(source, columns, jnp.zeros((8, cw), jnp.float32), landed=False)
            out = pltpu.make_async_copy(w, w_out, mine.at[4])
            out.start()
            out.wait()

    for copy in spreads:
        copy.wait_send()
    for p, peer in enumerate(peers):
        for c in range(pieces):
            if c == last and is_held(n, send_keys, p):

                @pl.when(middle == 1)
                def _():
                    block_copy(me, peer, c).wait_send()

            else:
                block_copy(me, peer, c).wait_send()
    for side in sides:
        for copy in side_copies(lane, side):
            copy.wait_send()
    if n == 8:

        @pl.when(middle == 0)
        def _():
            pl.semaphore_wait(go, len(CROSS))


def gather_and_serve(n, m, train, low, high, gain):
    rows, width = train.shape
    cols = width // n
    rank = low.shape[0]
    piece = gain.shape[1]
    q = m if rows % (128 * m) == 0 else 1
    cw = 128
    pieces = cols // cw
    dma = pltpu.SemaphoreType.DMA
    return pl.pallas_call(
        functools.partial(exchange, n, m, q, cw),
        out_shape=(
            pltpu.VMEM((n * rows, cols), train.dtype),
            pltpu.VMEM((1, cols), jnp.float32),
            pltpu.VMEM((n, m, 1, piece), jnp.float32),
            pltpu.VMEM((8, cw), jnp.float32),
            jax.ShapeDtypeStruct((n * rows, cw), jnp.float32),
        ),
        in_specs=[pl.BlockSpec(memory_space=pl.ANY)] * 4,
        out_specs=[pl.BlockSpec(memory_space=pltpu.VMEM)] * 4 + [pl.BlockSpec(memory_space=pl.ANY)],
        scratch_shapes=[
            pltpu.VMEM((q, n, rank, rows // q), low.dtype),
            pltpu.VMEM((m, n, 1, piece), jnp.float32),
            pltpu.VMEM((rank, cols), high.dtype),
            pltpu.VMEM((n * rows, cw), jnp.float32),
            dma((n, pieces)),
            dma((n, pieces)),
            dma((n,)),
            dma((n,)),
            dma((n,)),
            dma((n,)),
            dma((2, m)),
            dma((2, m)),
            dma((5,)),
            pltpu.SemaphoreType.REGULAR,
        ],
        compiler_params=pltpu.CompilerParams(collective_id=0, has_side_effects=True, vmem_limit_bytes=GRANT),
        name="exchange",
    )(*(pltpu.with_memory_space_constraint(x, pltpu.HBM) for x in (train, low, high, gain)))


def put_out(parts, whole, serving, sems):
    tall = whole.shape[0] // parts
    copies = [pltpu.make_async_copy(whole.at[pl.ds(i * tall, tall), :], serving.at[pl.ds(i * tall, tall), :], sems.at[i]) for i in range(parts)]
    for copy in copies:
        copy.start()
    for copy in copies:
        copy.wait()


def store(whole):
    parts = 12
    return pl.pallas_call(
        functools.partial(put_out, parts),
        out_shape=jax.ShapeDtypeStruct(whole.shape, whole.dtype),
        in_specs=[pl.BlockSpec(memory_space=pl.ANY)],
        out_specs=pl.BlockSpec(memory_space=pl.ANY),
        scratch_shapes=[pltpu.SemaphoreType.DMA((parts,))],
        compiler_params=pltpu.CompilerParams(vmem_limit_bytes=GRANT),
        name="store",
    )(pltpu.with_memory_space_constraint(whole, pltpu.VMEM))


def finish(n, cw, train, w_in, total, scale, stored, ended, scale_out, w, land, sends, recvs, mine):
    me = lax.axis_index("zero")
    rows = train.shape[0]
    cols = scale.shape[1]
    z = lax.div(me, 2)
    middle = lax.rem(lax.div(z, 2) + z, 2)
    peers = [partner(me, key, n) for key in HELD]
    columns = pl.ds(cols - cw, cw)
    tall = 256
    scale_out[...] = scale[...]

    @pl.when(middle == 0)
    def _():
        barrier = pltpu.get_barrier_semaphore()
        for peer in peers:
            pl.semaphore_signal(barrier, inc=1, device_id={"zero": peer}, device_id_type=MESH)
        pl.semaphore_wait(barrier, len(peers))
        copies = [
            pltpu.make_async_remote_copy(
                src_ref=train.at[:, pl.ds(pl.multiple_of(peer * cols + cols - cw, 128), cw)],
                dst_ref=land.at[i],
                send_sem=sends.at[i],
                recv_sem=recvs.at[i],
                device_id={"zero": peer},
                device_id_type=MESH,
            )
            for i, peer in enumerate(peers)
        ]
        for copy in copies:
            copy.start()
        fetch = pltpu.make_async_copy(w_in, w, mine)
        fetch.start()
        fetch.wait()

        def value(i, peer, t):
            a = pl.multiple_of(peer * rows + t * tall, tall)
            return land[i, pl.ds(pl.multiple_of(t * tall, tall), tall), :].astype(jnp.float32) + w[pl.ds(a, tall), :]

        summed = total[...]
        for i, peer in enumerate(peers):
            copies[i].wait_recv()

            def add_up(t, summed):
                return summed + jnp.sum(jnp.abs(value(i, peer, t)).reshape(tall // 8, 8, cw), axis=0)

            summed = lax.fori_loop(0, rows // tall, add_up, summed, unroll=2)
        mean = jnp.sum(summed, axis=0, keepdims=True) / (n * rows)
        scale_out[:, columns] = mean
        inverse = 1.0 / mean

        for key in range(n):
            if key in HELD:
                i = HELD.index(key)

                def divide(t, carry):
                    a = pl.multiple_of(peers[i] * rows + t * tall, tall)
                    ended[pl.ds(a, tall), :] = (value(i, peers[i], t) * inverse).astype(ended.dtype)
                    return carry

            else:
                source = partner(me, key, n)

                def divide(t, carry):
                    a = pl.multiple_of(source * rows + t * tall, tall)
                    ended[pl.ds(a, tall), :] = (w[pl.ds(a, tall), :] * inverse).astype(ended.dtype)
                    return carry

            lax.fori_loop(0, rows // tall, divide, 0, unroll=3)
        for copy in copies:
            copy.wait_send()


def end_columns(n, train, w, total, scale, stored):
    cw = w.shape[1]
    rows = train.shape[0]
    here = functools.partial(pltpu.with_memory_space_constraint, memory_space=pltpu.VMEM)
    there = functools.partial(pltpu.with_memory_space_constraint, memory_space=pltpu.HBM)
    return pl.pallas_call(
        functools.partial(finish, n, cw),
        out_shape=(pltpu.VMEM(w.shape, train.dtype), pltpu.VMEM(scale.shape, scale.dtype)),
        in_specs=[pl.BlockSpec(memory_space=pl.ANY)] * 2 + [pl.BlockSpec(memory_space=pltpu.VMEM)] * 2 + [pl.BlockSpec(memory_space=pl.ANY)],
        out_specs=[pl.BlockSpec(memory_space=pltpu.VMEM)] * 2,
        scratch_shapes=[pltpu.VMEM(w.shape, w.dtype), pltpu.VMEM((len(HELD), rows, cw), train.dtype), pltpu.SemaphoreType.DMA((2,)), pltpu.SemaphoreType.DMA((2,)), pltpu.SemaphoreType.DMA],
        compiler_params=pltpu.CompilerParams(collective_id=1, has_side_effects=True, vmem_limit_bytes=GRANT),
        name="finish",
    )(there(train), there(w), here(total), here(scale), there(stored))


def put_end(parts, stored, ended, out, sems):
    z = lax.div(lax.axis_index("zero"), 2)
    cw = ended.shape[1]
    tall = ended.shape[0] // parts
    columns = pl.ds(out.shape[1] - cw, cw)

    @pl.when(lax.rem(lax.div(z, 2) + z, 2) == 0)
    def _():
        copies = [pltpu.make_async_copy(ended.at[pl.ds(i * tall, tall), :], out.at[pl.ds(i * tall, tall), columns], sems.at[i]) for i in range(parts)]
        for copy in copies:
            copy.start()
        for copy in copies:
            copy.wait()


def store_end(stored, ended):
    parts = 12
    return pl.pallas_call(
        functools.partial(put_end, parts),
        out_shape=jax.ShapeDtypeStruct(stored.shape, stored.dtype),
        in_specs=[pl.BlockSpec(memory_space=pl.ANY)] * 2,
        out_specs=pl.BlockSpec(memory_space=pl.ANY),
        scratch_shapes=[pltpu.SemaphoreType.DMA((parts,))],
        input_output_aliases={0: 0},
        compiler_params=pltpu.CompilerParams(vmem_limit_bytes=GRANT),
        name="store_end",
    )(stored, pltpu.with_memory_space_constraint(ended, pltpu.VMEM))


def local(n, m, train_up, low_up, high_up, norm_train, norm_step):
    gain = (norm_train + norm_step).reshape(1, -1)
    whole, scale, norm, total, w = gather_and_serve(n, m, train_up, low_up.T, high_up, gain)
    serve_norm = norm.reshape(-1).astype(jnp.bfloat16)
    stored = store(whole)
    if n == 8:
        stored, serve_norm = lax.optimization_barrier((stored, serve_norm))
        ended, scale = end_columns(n, train_up, w, total, scale, stored)
        stored = store_end(stored, ended)
    return (stored, scale.reshape(-1), serve_norm)


def solution(mesh):
    in_specs = (
        P("zero", "model"),
        P("zero", None),
        P(None, "model"),
        P(("zero", "model")),
        P(("zero", "model")),
    )
    out_specs = (P(None, ("model", "zero")), P(("model", "zero")), P())
    body = functools.partial(local, mesh.shape["zero"], mesh.shape["model"])
    return jax.shard_map(body, mesh=mesh, in_specs=in_specs, out_specs=out_specs, check_vma=False)
```

```python
import functools

import jax
import jax.numpy as jnp
from jax import lax
from jax.experimental import pallas as pl
from jax.experimental.pallas import tpu as pltpu
from jax.sharding import PartitionSpec as P

mix_rate = 0.5
MESH = pl.DeviceIdType.MESH
GRANT = 16 * 2**20
HELD = (6, 7)
CROSS = (2, 3, 4, 5)
LEAD = 4
PAUSE = 6000


def bit(value, place):
    return lax.rem(lax.div(value, 2**place), 2)


def partner(me, key, n):
    other = 0
    for place in range(n.bit_length() - 1):
        a, b = bit(me, place), bit(key, place)
        other = other + 2**place * (a + b - 2 * a * b)
    return other


def send_order(n):
    far = list(range(n // 2, n))
    near = list(range(n // 2 - 1, 0, -1))
    order = []
    for i in range(len(far)):
        order.append(far[i])
        if i < len(near):
            order.append(near[i])
    return order


def orders(n):
    if n == 8:
        sends = ([6, 7, 4, 5, 2, 3, 1], [1, 2, 3, 4, 5, 6, 7])
        waits = ([6, 7, 2, 3, 1, 4, 5], [1, 4, 5, 2, 3, 6, 7])
        return sends, waits
    order = send_order(n)
    return (order, order), (order, order)


def key_at(order, place, middle):
    ends, mids = order[0][place], order[1][place]
    return ends if ends == mids else ends + middle * (mids - ends)


def is_held(n, order, place):
    return n == 8 and order[0][place] in HELD


def exchange(n, m, q, cw, train, low, high, gain, step, whole, scale, norm, total_out, w_out, lows, norms, highs, w, terms, sends, recvs, low_s, low_r, norm_s, norm_r, side_s, side_r, mine, go):
    me = lax.axis_index("zero")
    lane = lax.axis_index("model")
    rows = train.shape[0]
    cols = whole.shape[1]
    pieces = cols // cw
    share = rows // q
    z = lax.div(me, 2)
    middle = lax.rem(lax.div(z, 2) + z, 2)
    send_keys, wait_keys = orders(n)
    peers = [partner(me, key_at(send_keys, p, middle), n) for p in range(n - 1)]
    sources = [partner(me, key_at(wait_keys, p, middle), n) for p in range(n - 1)]
    sides = [lax.rem(lane + k, m) for k in range(1, m)]

    barrier = pltpu.get_barrier_semaphore()
    for peer in peers:
        pl.semaphore_signal(barrier, inc=1, device_id={"zero": peer}, device_id_type=MESH)
    for side in sides:
        pl.semaphore_signal(barrier, inc=1, device_id={"model": side}, device_id_type=MESH)

    own = [
        pltpu.make_async_copy(train.at[:, pl.ds(pl.multiple_of(me * cols, 128), cols)], whole.at[pl.ds(pl.multiple_of(me * rows, 128), rows), :], mine.at[0]),
        pltpu.make_async_copy(high.at[:, pl.ds(pl.multiple_of(me * cols, 128), cols)], highs, mine.at[1]),
    ]
    at = lane if q > 1 else 0
    low_part = low.at[:, pl.ds(pl.multiple_of(at * share, 128), share)]
    keep = [
        pltpu.make_async_copy(low_part, lows.at[at, me], mine.at[2]),
    ]
    load = [pltpu.make_async_copy(src, dst, mine.at[i]) for src, dst, i in ((gain, terms[0], 3), (step, terms[1], 5))]
    for copy in load + keep + own:
        copy.start()
    for copy in load:
        copy.wait()
    norms[lane, me] = (terms[0][...] + terms[1][...]).reshape(1, -1)
    pl.semaphore_wait(barrier, n + m - 2)

    def spread(i, origin, peer, fresh):
        refs = ((low_part, lows.at[at, origin], low_s, low_r), (norms.at[lane, origin], norms.at[lane, origin], norm_s, norm_r))
        return [
            pltpu.make_async_remote_copy(
                src_ref=src if fresh else dst, dst_ref=dst, send_sem=sent.at[i], recv_sem=came.at[origin], device_id={"zero": peer}, device_id_type=MESH
            )
            for src, dst, sent, came in refs
        ]

    def block_copy(origin, peer, c):
        return pltpu.make_async_remote_copy(
            src_ref=train.at[:, pl.ds(pl.multiple_of(peer * cols + c * cw, 128), cw)],
            dst_ref=whole.at[pl.ds(pl.multiple_of(origin * rows, 128), rows), pl.ds(pl.multiple_of(c * cw, 128), cw)],
            send_sem=sends.at[peer, c],
            recv_sem=recvs.at[origin, c],
            device_id={"zero": peer},
            device_id_type=MESH,
        )

    def side_copies(origin, side):
        pairs = [(norms.at[origin], norms.at[origin])]
        if q > 1:
            pairs.append((lows.at[origin], lows.at[origin]))
        return [
            pltpu.make_async_remote_copy(src_ref=src, dst_ref=dst, send_sem=side_s.at[i, side], recv_sem=side_r.at[i, origin], device_id={"model": side}, device_id_type=MESH)
            for i, (src, dst) in enumerate(pairs)
        ]

    spreads = spread(0, me, partner(me, n // 2, n), True)
    for copy in spreads:
        copy.start()
    last = pieces - 1
    for p, peer in enumerate(peers):
        for c in range(pieces):
            if c == last and is_held(n, send_keys, p):

                @pl.when(middle == 1)
                def _():
                    block_copy(me, peer, c).start()

            else:
                block_copy(me, peer, c).start()

    for copy in keep + own:
        copy.wait()
    held = [me]
    key = n // 2
    while key:
        peer = partner(me, key, n)
        if key < n // 2:
            for origin in held:
                copies = spread(len(spreads) // 2, origin, peer, False)
                for copy in copies:
                    copy.start()
                spreads += copies
        arrived = [partner(origin, key, n) for origin in held]
        for origin in arrived:
            for copy in spread(0, origin, peer, False):
                copy.wait_recv()
        held += arrived
        key //= 2
    for side in sides:
        for copy in side_copies(lane, side):
            copy.start()
    highs[...] = (mix_rate * highs[...].astype(jnp.float32)).astype(highs.dtype)
    for side in sides:
        for copy in side_copies(side, side):
            copy.wait_recv()

    for i in range(n):
        for j in range(m):
            norm[i, j] = norms[j, i]

    tall = 128
    per = share // tall
    far = 256 if rows % 256 == 0 else 128

    def merge(origin, columns, total, landed=True):
        high_tile = highs[:, columns]

        def add_up(t, total):
            a = pl.multiple_of(origin * rows + t * tall, tall)
            part = lows[lax.div(t, per), origin, :, pl.ds(pl.multiple_of(lax.rem(t, per) * tall, tall), tall)]
            new = lax.dot_general(part, high_tile, (((0,), (0,)), ((), ())), preferred_element_type=jnp.float32)
            if landed:
                new = whole[pl.ds(a, tall), columns].astype(jnp.float32) + new
            w[pl.ds(a, tall), :] = new
            return total + jnp.sum(jnp.abs(new).reshape(tall // 8, 8, cw), axis=0) if landed else total

        return lax.fori_loop(0, rows // tall, add_up, total, unroll=3)

    def finish_columns(columns, total):
        mean = jnp.sum(total, axis=0, keepdims=True) / (n * rows)
        scale[:, columns] = mean
        inverse = 1.0 / mean

        def divide(t, carry):
            a = pl.multiple_of(t * far, far)
            whole[pl.ds(a, far), columns] = (w[pl.ds(a, far), :] * inverse).astype(whole.dtype)
            return carry

        lax.fori_loop(0, n * rows // far, divide, 0, unroll=2)

    def piece(c, carry):
        columns = pl.ds(pl.multiple_of(c * cw, 128), cw)
        total = merge(me, columns, jnp.zeros((8, cw), jnp.float32))
        for source in sources:
            block_copy(source, source, c).wait_recv()
            total = merge(source, columns, total)
        if n == 8:

            @pl.when(jnp.logical_and(middle == 1, c == pieces - LEAD))
            def _():
                for key in CROSS:
                    pl.semaphore_signal(go, inc=1, device_id={"zero": partner(me, key, n)}, device_id_type=MESH)

        finish_columns(columns, total)
        return carry

    if n != 8:
        lax.fori_loop(0, pieces, piece, 0)
        total_out[...] = jnp.zeros_like(total_out)
    else:
        lax.fori_loop(0, last, piece, 0)
        columns = pl.ds(last * cw, cw)
        total = merge(me, columns, jnp.zeros((8, cw), jnp.float32))
        held = [source for p, source in enumerate(sources) if is_held(n, wait_keys, p)]
        for p, source in enumerate(sources):
            if not is_held(n, wait_keys, p):
                block_copy(source, source, last).wait_recv()
                total = merge(source, columns, total)
        total_out[...] = total

        @pl.when(middle == 1)
        def _():
            total = total_out[...]
            for source in held:
                block_copy(source, source, last).wait_recv()
                total = merge(source, columns, total)
            finish_columns(columns, total)

        @pl.when(middle == 0)
        def _():
            for source in held:
                merge(source, columns, jnp.zeros((8, cw), jnp.float32), landed=False)
            out = pltpu.make_async_copy(w, w_out, mine.at[4])
            out.start()
            out.wait()

    for copy in spreads:
        copy.wait_send()
    for p, peer in enumerate(peers):
        for c in range(pieces):
            if c == last and is_held(n, send_keys, p):

                @pl.when(middle == 1)
                def _():
                    block_copy(me, peer, c).wait_send()

            else:
                block_copy(me, peer, c).wait_send()
    for side in sides:
        for copy in side_copies(lane, side):
            copy.wait_send()
    if n == 8:

        @pl.when(middle == 0)
        def _():
            pl.semaphore_wait(go, len(CROSS))
            pl.delay(PAUSE)


def gather_and_serve(n, m, train, low, high, gain, step):
    rows, width = train.shape
    cols = width // n
    rank = low.shape[0]
    piece = gain.shape[0]
    q = m if rows % (128 * m) == 0 else 1
    cw = 128
    pieces = cols // cw
    dma = pltpu.SemaphoreType.DMA
    return pl.pallas_call(
        functools.partial(exchange, n, m, q, cw),
        out_shape=(
            pltpu.VMEM((n * rows, cols), train.dtype),
            pltpu.VMEM((1, cols), jnp.float32),
            pltpu.VMEM((n, m, 1, piece), jnp.float32),
            pltpu.VMEM((8, cw), jnp.float32),
            jax.ShapeDtypeStruct((n * rows, cw), jnp.float32),
        ),
        in_specs=[pl.BlockSpec(memory_space=pl.ANY)] * 5,
        out_specs=[pl.BlockSpec(memory_space=pltpu.VMEM)] * 4 + [pl.BlockSpec(memory_space=pl.ANY)],
        scratch_shapes=[
            pltpu.VMEM((q, n, rank, rows // q), low.dtype),
            pltpu.VMEM((m, n, 1, piece), jnp.float32),
            pltpu.VMEM((rank, cols), high.dtype),
            pltpu.VMEM((n * rows, cw), jnp.float32),
            [pltpu.VMEM((piece,), jnp.float32)] * 2,
            dma((n, pieces)),
            dma((n, pieces)),
            dma((n,)),
            dma((n,)),
            dma((n,)),
            dma((n,)),
            dma((2, m)),
            dma((2, m)),
            dma((6,)),
            pltpu.SemaphoreType.REGULAR,
        ],
        compiler_params=pltpu.CompilerParams(collective_id=0, has_side_effects=True, vmem_limit_bytes=GRANT),
        name="exchange",
    )(*(pltpu.with_memory_space_constraint(x, pltpu.HBM) for x in (train, low, high, gain, step)))


def put_out(parts, whole, serving, sems):
    tall = whole.shape[0] // parts
    copies = [pltpu.make_async_copy(whole.at[pl.ds(i * tall, tall), :], serving.at[pl.ds(i * tall, tall), :], sems.at[i]) for i in range(parts)]
    for copy in copies:
        copy.start()
    for copy in copies:
        copy.wait()


def store(whole):
    parts = 12
    return pl.pallas_call(
        functools.partial(put_out, parts),
        out_shape=jax.ShapeDtypeStruct(whole.shape, whole.dtype),
        in_specs=[pl.BlockSpec(memory_space=pl.ANY)],
        out_specs=pl.BlockSpec(memory_space=pl.ANY),
        scratch_shapes=[pltpu.SemaphoreType.DMA((parts,))],
        compiler_params=pltpu.CompilerParams(vmem_limit_bytes=GRANT),
        name="store",
    )(pltpu.with_memory_space_constraint(whole, pltpu.VMEM))


def finish(n, cw, train, w_in, total, scale, stored, ended, scale_out, w, land, sends, recvs, mine):
    me = lax.axis_index("zero")
    rows = train.shape[0]
    cols = scale.shape[1]
    z = lax.div(me, 2)
    middle = lax.rem(lax.div(z, 2) + z, 2)
    peers = [partner(me, key, n) for key in HELD]
    columns = pl.ds(cols - cw, cw)
    tall = 256
    scale_out[...] = scale[...].reshape(scale_out.shape)

    @pl.when(middle == 0)
    def _():
        barrier = pltpu.get_barrier_semaphore()
        for peer in peers:
            pl.semaphore_signal(barrier, inc=1, device_id={"zero": peer}, device_id_type=MESH)
        pl.semaphore_wait(barrier, len(peers))
        copies = [
            pltpu.make_async_remote_copy(
                src_ref=train.at[:, pl.ds(pl.multiple_of(peer * cols + cols - cw, 128), cw)],
                dst_ref=land.at[i],
                send_sem=sends.at[i],
                recv_sem=recvs.at[i],
                device_id={"zero": peer},
                device_id_type=MESH,
            )
            for i, peer in enumerate(peers)
        ]
        for copy in copies:
            copy.start()
        fetch = pltpu.make_async_copy(w_in, w, mine)
        fetch.start()
        fetch.wait()

        def value(i, peer, t):
            a = pl.multiple_of(peer * rows + t * tall, tall)
            return land[i, pl.ds(pl.multiple_of(t * tall, tall), tall), :].astype(jnp.float32) + w[pl.ds(a, tall), :]

        summed = total[...]
        for i, peer in enumerate(peers):
            copies[i].wait_recv()

            def add_up(t, summed):
                return summed + jnp.sum(jnp.abs(value(i, peer, t)).reshape(tall // 8, 8, cw), axis=0)

            summed = lax.fori_loop(0, rows // tall, add_up, summed, unroll=2)
        mean = jnp.sum(summed, axis=0, keepdims=True) / (n * rows)
        scale_out[columns] = mean.reshape(cw)
        inverse = 1.0 / mean

        for key in range(n):
            if key in HELD:
                i = HELD.index(key)

                def divide(t, carry):
                    a = pl.multiple_of(peers[i] * rows + t * tall, tall)
                    ended[pl.ds(a, tall), :] = (value(i, peers[i], t) * inverse).astype(ended.dtype)
                    return carry

            else:
                source = partner(me, key, n)

                def divide(t, carry):
                    a = pl.multiple_of(source * rows + t * tall, tall)
                    ended[pl.ds(a, tall), :] = (w[pl.ds(a, tall), :] * inverse).astype(ended.dtype)
                    return carry

            lax.fori_loop(0, rows // tall, divide, 0, unroll=3)
        for copy in copies:
            copy.wait_send()


def end_columns(n, train, w, total, scale, stored):
    cw = w.shape[1]
    rows = train.shape[0]
    here = functools.partial(pltpu.with_memory_space_constraint, memory_space=pltpu.VMEM)
    there = functools.partial(pltpu.with_memory_space_constraint, memory_space=pltpu.HBM)
    return pl.pallas_call(
        functools.partial(finish, n, cw),
        out_shape=(pltpu.VMEM(w.shape, train.dtype), pltpu.VMEM(scale.shape[1:], scale.dtype)),
        in_specs=[pl.BlockSpec(memory_space=pl.ANY)] * 2 + [pl.BlockSpec(memory_space=pltpu.VMEM)] * 2 + [pl.BlockSpec(memory_space=pl.ANY)],
        out_specs=[pl.BlockSpec(memory_space=pltpu.VMEM)] * 2,
        scratch_shapes=[pltpu.VMEM(w.shape, w.dtype), pltpu.VMEM((len(HELD), rows, cw), train.dtype), pltpu.SemaphoreType.DMA((2,)), pltpu.SemaphoreType.DMA((2,)), pltpu.SemaphoreType.DMA],
        compiler_params=pltpu.CompilerParams(collective_id=1, has_side_effects=True, vmem_limit_bytes=GRANT),
        name="finish",
    )(there(train), there(w), here(total), here(scale), there(stored))


def put_end(parts, stored, ended, scale, out, scale_out, sems):
    z = lax.div(lax.axis_index("zero"), 2)
    cw = ended.shape[1]
    tall = ended.shape[0] // parts
    columns = pl.ds(out.shape[1] - cw, cw)
    put_scale = pltpu.make_async_copy(scale, scale_out, sems.at[parts])
    put_scale.start()

    @pl.when(lax.rem(lax.div(z, 2) + z, 2) == 0)
    def _():
        copies = [pltpu.make_async_copy(ended.at[pl.ds(i * tall, tall), :], out.at[pl.ds(i * tall, tall), columns], sems.at[i]) for i in range(parts)]
        for copy in copies:
            copy.start()
        for copy in copies:
            copy.wait()

    put_scale.wait()


def store_end(stored, ended, scale):
    parts = 12
    return pl.pallas_call(
        functools.partial(put_end, parts),
        out_shape=(jax.ShapeDtypeStruct(stored.shape, stored.dtype), jax.ShapeDtypeStruct(scale.shape, scale.dtype)),
        in_specs=[pl.BlockSpec(memory_space=pl.ANY)] * 3,
        out_specs=[pl.BlockSpec(memory_space=pl.ANY)] * 2,
        scratch_shapes=[pltpu.SemaphoreType.DMA((parts + 1,))],
        input_output_aliases={0: 0},
        compiler_params=pltpu.CompilerParams(vmem_limit_bytes=GRANT),
        name="store_end",
    )(stored, pltpu.with_memory_space_constraint(ended, pltpu.VMEM), pltpu.with_memory_space_constraint(scale, pltpu.VMEM))


def local(n, m, train_up, low_up, high_up, norm_train, norm_step):
    whole, scale, norm, total, w = gather_and_serve(n, m, train_up, low_up.T, high_up, norm_train, norm_step)
    serve_norm = norm.reshape(-1).astype(jnp.bfloat16)
    stored = store(whole)
    if n == 8:
        stored, serve_norm = lax.optimization_barrier((stored, serve_norm))
        ended, scale = end_columns(n, train_up, w, total, scale, stored)
        stored, scale = store_end(stored, ended, scale)
    return (stored, scale.reshape(-1), serve_norm)


def solution(mesh):
    in_specs = (
        P("zero", "model"),
        P("zero", None),
        P(None, "model"),
        P(("zero", "model")),
        P(("zero", "model")),
    )
    out_specs = (P(None, ("model", "zero")), P(("model", "zero")), P())
    body = functools.partial(local, mesh.shape["zero"], mesh.shape["model"])
    return jax.shard_map(body, mesh=mesh, in_specs=in_specs, out_specs=out_specs, check_vma=False)
```

```python
import functools

import jax
import jax.numpy as jnp
from jax import lax
from jax.experimental import pallas as pl
from jax.experimental.pallas import tpu as pltpu
from jax.sharding import PartitionSpec as P

mix_rate = 0.5
MESH = pl.DeviceIdType.MESH
GRANT = 16 * 2**20
HELD = (6, 7)
CROSS = (2, 3, 4, 5)
LEAD = 4
PAUSE = 5500


def bit(value, place):
    return lax.rem(lax.div(value, 2**place), 2)


def partner(me, key, n):
    other = 0
    for place in range(n.bit_length() - 1):
        a, b = bit(me, place), bit(key, place)
        other = other + 2**place * (a + b - 2 * a * b)
    return other


def send_order(n):
    far = list(range(n // 2, n))
    near = list(range(n // 2 - 1, 0, -1))
    order = []
    for i in range(len(far)):
        order.append(far[i])
        if i < len(near):
            order.append(near[i])
    return order


def orders(n):
    if n == 8:
        sends = ([6, 7, 4, 5, 2, 3, 1], [1, 2, 3, 4, 5, 6, 7])
        waits = ([6, 7, 2, 3, 1, 4, 5], [1, 4, 5, 2, 3, 6, 7])
        return sends, waits
    order = send_order(n)
    return (order, order), (order, order)


def key_at(order, place, middle):
    ends, mids = order[0][place], order[1][place]
    return ends if ends == mids else ends + middle * (mids - ends)


def is_held(n, order, place):
    return n == 8 and order[0][place] in HELD


def exchange(n, m, q, cw, train, low, high, gain, step, whole, scale, norm, total_out, w_out, lows, norms, highs, w, terms, sends, recvs, low_s, low_r, norm_s, norm_r, side_s, side_r, mine, go):
    me = lax.axis_index("zero")
    lane = lax.axis_index("model")
    rows = train.shape[0]
    cols = whole.shape[1]
    pieces = cols // cw
    share = rows // q
    z = lax.div(me, 2)
    middle = lax.rem(lax.div(z, 2) + z, 2)
    send_keys, wait_keys = orders(n)
    peers = [partner(me, key_at(send_keys, p, middle), n) for p in range(n - 1)]
    sources = [partner(me, key_at(wait_keys, p, middle), n) for p in range(n - 1)]
    sides = [lax.rem(lane + k, m) for k in range(1, m)]

    barrier = pltpu.get_barrier_semaphore()
    for peer in peers:
        pl.semaphore_signal(barrier, inc=1, device_id={"zero": peer}, device_id_type=MESH)
    for side in sides:
        pl.semaphore_signal(barrier, inc=1, device_id={"model": side}, device_id_type=MESH)

    own = [
        pltpu.make_async_copy(train.at[:, pl.ds(pl.multiple_of(me * cols, 128), cols)], whole.at[pl.ds(pl.multiple_of(me * rows, 128), rows), :], mine.at[0]),
        pltpu.make_async_copy(high.at[:, pl.ds(pl.multiple_of(me * cols, 128), cols)], highs, mine.at[1]),
    ]
    at = lane if q > 1 else 0
    low_part = low.at[:, pl.ds(pl.multiple_of(at * share, 128), share)]
    keep = [
        pltpu.make_async_copy(low_part, lows.at[at, me], mine.at[2]),
    ]
    load = [pltpu.make_async_copy(src, dst, mine.at[i]) for src, dst, i in ((gain, terms[0], 3), (step, terms[1], 5))]
    for copy in load + keep + own:
        copy.start()
    for copy in load:
        copy.wait()
    norms[lane, me] = (terms[0][...] + terms[1][...]).reshape(1, -1)
    pl.semaphore_wait(barrier, n + m - 2)

    def spread(i, origin, peer, fresh):
        refs = ((low_part, lows.at[at, origin], low_s, low_r), (norms.at[lane, origin], norms.at[lane, origin], norm_s, norm_r))
        return [
            pltpu.make_async_remote_copy(
                src_ref=src if fresh else dst, dst_ref=dst, send_sem=sent.at[i], recv_sem=came.at[origin], device_id={"zero": peer}, device_id_type=MESH
            )
            for src, dst, sent, came in refs
        ]

    def block_copy(origin, peer, c):
        return pltpu.make_async_remote_copy(
            src_ref=train.at[:, pl.ds(pl.multiple_of(peer * cols + c * cw, 128), cw)],
            dst_ref=whole.at[pl.ds(pl.multiple_of(origin * rows, 128), rows), pl.ds(pl.multiple_of(c * cw, 128), cw)],
            send_sem=sends.at[peer, c],
            recv_sem=recvs.at[origin, c],
            device_id={"zero": peer},
            device_id_type=MESH,
        )

    def side_copies(origin, side):
        pairs = [(norms.at[origin], norms.at[origin])]
        if q > 1:
            pairs.append((lows.at[origin], lows.at[origin]))
        return [
            pltpu.make_async_remote_copy(src_ref=src, dst_ref=dst, send_sem=side_s.at[i, side], recv_sem=side_r.at[i, origin], device_id={"model": side}, device_id_type=MESH)
            for i, (src, dst) in enumerate(pairs)
        ]

    spreads = spread(0, me, partner(me, n // 2, n), True)
    for copy in spreads:
        copy.start()
    last = pieces - 1
    for p, peer in enumerate(peers):
        for c in range(pieces):
            if c == last and is_held(n, send_keys, p):

                @pl.when(middle == 1)
                def _():
                    block_copy(me, peer, c).start()

            else:
                block_copy(me, peer, c).start()

    for copy in keep + own:
        copy.wait()
    held = [me]
    key = n // 2
    while key:
        peer = partner(me, key, n)
        if key < n // 2:
            for origin in held:
                copies = spread(len(spreads) // 2, origin, peer, False)
                for copy in copies:
                    copy.start()
                spreads += copies
        arrived = [partner(origin, key, n) for origin in held]
        for origin in arrived:
            for copy in spread(0, origin, peer, False):
                copy.wait_recv()
        held += arrived
        key //= 2
    for side in sides:
        for copy in side_copies(lane, side):
            copy.start()
    highs[...] = (mix_rate * highs[...].astype(jnp.float32)).astype(highs.dtype)
    for side in sides:
        for copy in side_copies(side, side):
            copy.wait_recv()

    for i in range(n):
        for j in range(m):
            norm[i, j] = norms[j, i]

    tall = 128
    per = share // tall
    far = 256 if rows % 256 == 0 else 128

    def merge(origin, columns, total, landed=True):
        high_tile = highs[:, columns]

        def add_up(t, total):
            a = pl.multiple_of(origin * rows + t * tall, tall)
            part = lows[lax.div(t, per), origin, :, pl.ds(pl.multiple_of(lax.rem(t, per) * tall, tall), tall)]
            new = lax.dot_general(part, high_tile, (((0,), (0,)), ((), ())), preferred_element_type=jnp.float32)
            if landed:
                new = whole[pl.ds(a, tall), columns].astype(jnp.float32) + new
            w[pl.ds(a, tall), :] = new
            return total + jnp.sum(jnp.abs(new).reshape(tall // 8, 8, cw), axis=0) if landed else total

        return lax.fori_loop(0, rows // tall, add_up, total, unroll=3)

    def finish_columns(columns, total):
        mean = jnp.sum(total, axis=0, keepdims=True) / (n * rows)
        scale[:, columns] = mean
        inverse = 1.0 / mean

        def divide(t, carry):
            a = pl.multiple_of(t * far, far)
            whole[pl.ds(a, far), columns] = (w[pl.ds(a, far), :] * inverse).astype(whole.dtype)
            return carry

        lax.fori_loop(0, n * rows // far, divide, 0, unroll=2)

    def piece(c, carry):
        columns = pl.ds(pl.multiple_of(c * cw, 128), cw)
        total = merge(me, columns, jnp.zeros((8, cw), jnp.float32))
        for source in sources:
            block_copy(source, source, c).wait_recv()
            total = merge(source, columns, total)
        if n == 8:

            @pl.when(jnp.logical_and(middle == 1, c == pieces - LEAD))
            def _():
                for key in CROSS:
                    pl.semaphore_signal(go, inc=1, device_id={"zero": partner(me, key, n)}, device_id_type=MESH)

        finish_columns(columns, total)
        return carry

    if n != 8:
        lax.fori_loop(0, pieces, piece, 0)
        total_out[...] = jnp.zeros_like(total_out)
    else:
        lax.fori_loop(0, last, piece, 0)
        columns = pl.ds(last * cw, cw)
        total = merge(me, columns, jnp.zeros((8, cw), jnp.float32))
        held = [source for p, source in enumerate(sources) if is_held(n, wait_keys, p)]
        for p, source in enumerate(sources):
            if not is_held(n, wait_keys, p):
                block_copy(source, source, last).wait_recv()
                total = merge(source, columns, total)
        total_out[...] = total

        @pl.when(middle == 1)
        def _():
            total = total_out[...]
            for source in held:
                block_copy(source, source, last).wait_recv()
                total = merge(source, columns, total)
            finish_columns(columns, total)

        @pl.when(middle == 0)
        def _():
            for source in held:
                merge(source, columns, jnp.zeros((8, cw), jnp.float32), landed=False)
            out = pltpu.make_async_copy(w, w_out, mine.at[4])
            out.start()
            out.wait()

    for copy in spreads:
        copy.wait_send()
    for p, peer in enumerate(peers):
        for c in range(pieces):
            if c == last and is_held(n, send_keys, p):

                @pl.when(middle == 1)
                def _():
                    block_copy(me, peer, c).wait_send()

            else:
                block_copy(me, peer, c).wait_send()
    for side in sides:
        for copy in side_copies(lane, side):
            copy.wait_send()
    if n == 8:

        @pl.when(middle == 0)
        def _():
            pl.semaphore_wait(go, len(CROSS))
            pl.delay(PAUSE)


def gather_and_serve(n, m, train, low, high, gain, step):
    rows, width = train.shape
    cols = width // n
    rank = low.shape[0]
    piece = gain.shape[0]
    q = m if rows % (128 * m) == 0 else 1
    cw = 128
    pieces = cols // cw
    dma = pltpu.SemaphoreType.DMA
    return pl.pallas_call(
        functools.partial(exchange, n, m, q, cw),
        out_shape=(
            pltpu.VMEM((n * rows, cols), train.dtype),
            pltpu.VMEM((1, cols), jnp.float32),
            pltpu.VMEM((n, m, 1, piece), jnp.float32),
            pltpu.VMEM((8, cw), jnp.float32),
            jax.ShapeDtypeStruct((n * rows, cw), jnp.float32),
        ),
        in_specs=[pl.BlockSpec(memory_space=pl.ANY)] * 5,
        out_specs=[pl.BlockSpec(memory_space=pltpu.VMEM)] * 4 + [pl.BlockSpec(memory_space=pl.ANY)],
        scratch_shapes=[
            pltpu.VMEM((q, n, rank, rows // q), low.dtype),
            pltpu.VMEM((m, n, 1, piece), jnp.float32),
            pltpu.VMEM((rank, cols), high.dtype),
            pltpu.VMEM((n * rows, cw), jnp.float32),
            [pltpu.VMEM((piece,), jnp.float32)] * 2,
            dma((n, pieces)),
            dma((n, pieces)),
            dma((n,)),
            dma((n,)),
            dma((n,)),
            dma((n,)),
            dma((2, m)),
            dma((2, m)),
            dma((6,)),
            pltpu.SemaphoreType.REGULAR,
        ],
        compiler_params=pltpu.CompilerParams(collective_id=0, has_side_effects=True, vmem_limit_bytes=GRANT),
        name="exchange",
    )(*(pltpu.with_memory_space_constraint(x, pltpu.HBM) for x in (train, low, high, gain, step)))


def put_out(parts, whole, serving, sems):
    tall = whole.shape[0] // parts
    copies = [pltpu.make_async_copy(whole.at[pl.ds(i * tall, tall), :], serving.at[pl.ds(i * tall, tall), :], sems.at[i]) for i in range(parts)]
    for copy in copies:
        copy.start()
    for copy in copies:
        copy.wait()


def store(whole):
    parts = 12
    return pl.pallas_call(
        functools.partial(put_out, parts),
        out_shape=jax.ShapeDtypeStruct(whole.shape, whole.dtype),
        in_specs=[pl.BlockSpec(memory_space=pl.ANY)],
        out_specs=pl.BlockSpec(memory_space=pl.ANY),
        scratch_shapes=[pltpu.SemaphoreType.DMA((parts,))],
        compiler_params=pltpu.CompilerParams(vmem_limit_bytes=GRANT),
        name="store",
    )(pltpu.with_memory_space_constraint(whole, pltpu.VMEM))


def finish(n, cw, train, w_in, total, scale, stored, ended, scale_out, w, land, sends, recvs, mine):
    me = lax.axis_index("zero")
    rows = train.shape[0]
    cols = scale.shape[1]
    z = lax.div(me, 2)
    middle = lax.rem(lax.div(z, 2) + z, 2)
    peers = [partner(me, key, n) for key in HELD]
    columns = pl.ds(cols - cw, cw)
    tall = 256
    scale_out[...] = scale[...].reshape(scale_out.shape)

    @pl.when(middle == 0)
    def _():
        barrier = pltpu.get_barrier_semaphore()
        for peer in peers:
            pl.semaphore_signal(barrier, inc=1, device_id={"zero": peer}, device_id_type=MESH)
        pl.semaphore_wait(barrier, len(peers))
        copies = [
            pltpu.make_async_remote_copy(
                src_ref=train.at[:, pl.ds(pl.multiple_of(peer * cols + cols - cw, 128), cw)],
                dst_ref=land.at[i],
                send_sem=sends.at[i],
                recv_sem=recvs.at[i],
                device_id={"zero": peer},
                device_id_type=MESH,
            )
            for i, peer in enumerate(peers)
        ]
        for copy in copies:
            copy.start()
        fetch = pltpu.make_async_copy(w_in, w, mine)
        fetch.start()
        fetch.wait()

        def value(i, peer, t):
            a = pl.multiple_of(peer * rows + t * tall, tall)
            return land[i, pl.ds(pl.multiple_of(t * tall, tall), tall), :].astype(jnp.float32) + w[pl.ds(a, tall), :]

        summed = total[...]
        for i, peer in enumerate(peers):
            copies[i].wait_recv()

            def add_up(t, summed):
                return summed + jnp.sum(jnp.abs(value(i, peer, t)).reshape(tall // 8, 8, cw), axis=0)

            summed = lax.fori_loop(0, rows // tall, add_up, summed, unroll=2)
        mean = jnp.sum(summed, axis=0, keepdims=True) / (n * rows)
        scale_out[columns] = mean.reshape(cw)
        inverse = 1.0 / mean

        for key in range(n):
            if key in HELD:
                i = HELD.index(key)

                def divide(t, carry):
                    a = pl.multiple_of(peers[i] * rows + t * tall, tall)
                    ended[pl.ds(a, tall), :] = (value(i, peers[i], t) * inverse).astype(ended.dtype)
                    return carry

            else:
                source = partner(me, key, n)

                def divide(t, carry):
                    a = pl.multiple_of(source * rows + t * tall, tall)
                    ended[pl.ds(a, tall), :] = (w[pl.ds(a, tall), :] * inverse).astype(ended.dtype)
                    return carry

            lax.fori_loop(0, rows // tall, divide, 0, unroll=3)
        for copy in copies:
            copy.wait_send()


def end_columns(n, train, w, total, scale, stored):
    cw = w.shape[1]
    rows = train.shape[0]
    here = functools.partial(pltpu.with_memory_space_constraint, memory_space=pltpu.VMEM)
    there = functools.partial(pltpu.with_memory_space_constraint, memory_space=pltpu.HBM)
    return pl.pallas_call(
        functools.partial(finish, n, cw),
        out_shape=(pltpu.VMEM(w.shape, train.dtype), pltpu.VMEM(scale.shape[1:], scale.dtype)),
        in_specs=[pl.BlockSpec(memory_space=pl.ANY)] * 2 + [pl.BlockSpec(memory_space=pltpu.VMEM)] * 2 + [pl.BlockSpec(memory_space=pl.ANY)],
        out_specs=[pl.BlockSpec(memory_space=pltpu.VMEM)] * 2,
        scratch_shapes=[pltpu.VMEM(w.shape, w.dtype), pltpu.VMEM((len(HELD), rows, cw), train.dtype), pltpu.SemaphoreType.DMA((2,)), pltpu.SemaphoreType.DMA((2,)), pltpu.SemaphoreType.DMA],
        compiler_params=pltpu.CompilerParams(collective_id=1, has_side_effects=True, vmem_limit_bytes=GRANT),
        name="finish",
    )(there(train), there(w), here(total), here(scale), there(stored))


def put_end(parts, stored, ended, scale, out, scale_out, sems):
    z = lax.div(lax.axis_index("zero"), 2)
    cw = ended.shape[1]
    tall = ended.shape[0] // parts
    columns = pl.ds(out.shape[1] - cw, cw)
    put_scale = pltpu.make_async_copy(scale, scale_out, sems.at[parts])
    put_scale.start()

    @pl.when(lax.rem(lax.div(z, 2) + z, 2) == 0)
    def _():
        copies = [pltpu.make_async_copy(ended.at[pl.ds(i * tall, tall), :], out.at[pl.ds(i * tall, tall), columns], sems.at[i]) for i in range(parts)]
        for copy in copies:
            copy.start()
        for copy in copies:
            copy.wait()

    put_scale.wait()


def store_end(stored, ended, scale):
    parts = 12
    return pl.pallas_call(
        functools.partial(put_end, parts),
        out_shape=(jax.ShapeDtypeStruct(stored.shape, stored.dtype), jax.ShapeDtypeStruct(scale.shape, scale.dtype)),
        in_specs=[pl.BlockSpec(memory_space=pl.ANY)] * 3,
        out_specs=[pl.BlockSpec(memory_space=pl.ANY)] * 2,
        scratch_shapes=[pltpu.SemaphoreType.DMA((parts + 1,))],
        input_output_aliases={0: 0},
        compiler_params=pltpu.CompilerParams(vmem_limit_bytes=GRANT),
        name="store_end",
    )(stored, pltpu.with_memory_space_constraint(ended, pltpu.VMEM), pltpu.with_memory_space_constraint(scale, pltpu.VMEM))


def local(n, m, train_up, low_up, high_up, norm_train, norm_step):
    whole, scale, norm, total, w = gather_and_serve(n, m, train_up, low_up.T, high_up, norm_train, norm_step)
    serve_norm = norm.reshape(-1).astype(jnp.bfloat16)
    stored = store(whole)
    if n == 8:
        stored, serve_norm = lax.optimization_barrier((stored, serve_norm))
        ended, scale = end_columns(n, train_up, w, total, scale, stored)
        stored, scale = store_end(stored, ended, scale)
    return (stored, scale.reshape(-1), serve_norm)


def solution(mesh):
    in_specs = (
        P("zero", "model"),
        P("zero", None),
        P(None, "model"),
        P(("zero", "model")),
        P(("zero", "model")),
    )
    out_specs = (P(None, ("model", "zero")), P(("model", "zero")), P())
    body = functools.partial(local, mesh.shape["zero"], mesh.shape["model"])
    return jax.shard_map(body, mesh=mesh, in_specs=in_specs, out_specs=out_specs, check_vma=False)
```
